512 devices in a mesh: row: 16 (over z, core), col: 4 (over x), depth: 8 (over y).
Axes of the slice: x: 4, y: 8, z: 8, core: 2. Of those that a mesh axis runs over, the one named last changes fastest.
Arguments:
- intersection_re: bfloat16 [8, 4096, 4096], P('depth', ('row', 'col')), may hold values from -1 to 1, as said below
- intersection_im: bfloat16 [8, 4096, 4096], P('depth', ('row', 'col')), may hold values from -1 to 1, as said below
- weights: float32 [8], replicated, may hold values from 0.5 to 2
- shells: int32 [8, 3], replicated, may hold values from -2 to 2
- rotation: bfloat16 [4096, 4096], P(('row', 'col')), may hold values from -6 to 6
Outputs:
- updated: float32 [4096, 4096], P(('row', 'col'), 'depth')
The draws below stay inside these ranges and needn't reach their ends.
Inputs may be any that keep to these rules, and one draw needn't show every extreme that they name: `intersection_re`: diagonal entries lie in 0.5 to 1. `intersection_im`: diagonal entries lie in -0.6 to 0.6.
All inputs are finite; a program needn't handle non-finite values.
Results may differ from the reference program's by a relative error of at most 0.035.
Values may be sent and summed in bfloat16 or wider, within the bound.
No kernel may reach another device: no remote copies, remote signals or barrier semaphores. Data moves between devices by JAX's collectives and lax.ppermute only.
A program may use at most 64 MiB of HBM per device.

```python
import math
import jax
import jax.numpy as jnp

WF = 4096
TERMS = 8
B = 8


def intersection_common(key, diag_lo, diag_hi):
    base_key, diag_key = jax.random.split(key, 2)
    values = jax.random.normal(base_key, (B, WF, WF), jnp.float32)
    values = values * WF ** (-0.5)
    diagonal = jax.random.uniform(diag_key, (B, WF), jnp.float32, diag_lo, diag_hi)
    index = jnp.arange(WF)
    values = values.at[:, index, index].set(diagonal)
    return values.astype(jnp.bfloat16)


def draw_intersection_re(key, part):
    return intersection_common(jax.random.fold_in(key, 11), 0.5, 1.0)


def draw_intersection_im(key, part):
    return intersection_common(jax.random.fold_in(key, 23), -0.6, 0.6)


def plant(entries, own_key, least, high):
    dims = entries.shape
    index_at = [jax.random.randint(jax.random.fold_in(own_key, axis), (), 0, dims[axis]) for axis in range(len(dims))]
    entries = entries.at[tuple(index_at)].set(least)
    longest = dims.index(max(dims))
    index_at[longest] = (index_at[longest] + 1) % dims[longest]
    return entries.at[tuple(index_at)].set(high)


def level_of(stream_key, shape, cuts, least, high):
    def one(axis_at, shards_of):
        draws = jax.random.uniform(jax.random.fold_in(jax.random.fold_in(stream_key, 6), axis_at), (shards_of,), jnp.float32, least / len(cuts), high / len(cuts))
        return jnp.repeat(jnp.exp(draws), shape[axis_at] // shards_of).reshape((-1,) + (1,) * (len(shape) - axis_at - 1))

    factor_of = one(*cuts[0])
    for cut in cuts[1:]:
        factor_of = factor_of * one(*cut)
    return factor_of


def noise(rng, shape, deviation, bound, shards=(), dtype=jnp.bfloat16):
    entries = deviation * jax.random.normal(rng, shape, jnp.float32)
    if shards:
        entries = entries * level_of(rng, shape, shards, -0.22, 0.18)
    return jnp.clip(entries, -bound, bound).astype(dtype)


def setup_inputs(seed: int = 0) -> dict:
    key_list = jax.random.split(jax.random.key(seed), 6)
    return {
        "intersection_re": draw_intersection_re(jax.random.fold_in(key_list[5], 71), 0),
        "intersection_im": draw_intersection_im(jax.random.fold_in(key_list[5], 71), 0),
        "weights": jnp.clip(jnp.exp(jax.random.uniform(key_list[2], (B,), jnp.float32, math.log(0.5), math.log(2.0))), 0.5, 2.0),
        "shells": plant(jax.random.randint(key_list[3], (B, 3), -2, 3), jax.random.fold_in(key_list[3], 1), -2, 2).astype(jnp.int32),
        "rotation": noise(key_list[4], (WF, WF), 0.5, 6.0, ((0, 64),)),
    }


LATTICE = 0.25

def reference(intersection_re, intersection_im, weights, shells, rotation):
    index = jnp.arange(WF)
    diag_re = intersection_re[:, index, index].astype(jnp.float32)
    diag_im = intersection_im[:, index, index].astype(jnp.float32)
    phase = jnp.arctan2(diag_im, diag_re)
    vectors = shells.astype(jnp.float32) * LATTICE
    centre = -jnp.einsum('bk,bn->kn', weights[:, None] * vectors, phase)
    spread = phase + jnp.einsum('bk,kn->bn', vectors, centre)
    modulus = diag_re * diag_re + diag_im * diag_im
    summed = jnp.zeros((WF, WF), jnp.float32)
    for shell in range(B):
        values_re = intersection_re[shell].astype(jnp.float32)
        values_im = intersection_im[shell].astype(jnp.float32)
        terms = values_re * diag_re[shell][None, :] + values_im * diag_im[shell][None, :]
        terms = terms - spread[shell][None, :] * (values_im * diag_re[shell][None, :] - values_re * diag_im[shell][None, :]) / modulus[shell][None, :]
        summed = summed + weights[shell] * terms
    factor = 1.25 / math.sqrt(B)
    generator = ((summed - summed.T) * factor).astype(jnp.bfloat16)
    series_term = rotation
    accum = rotation.astype(jnp.float32)
    for order in range(1, TERMS):
        product = jnp.dot(series_term, generator, preferred_element_type=jnp.float32)
        series_term = (product / order).astype(jnp.bfloat16)
        accum = accum + series_term.astype(jnp.float32)
    return accum
```

```python
import functools
import math

import jax
import jax.numpy as jnp
from jax import lax
from jax.experimental import pallas as pl
from jax.experimental.pallas import tpu as pltpu
from jax.sharding import Mesh, PartitionSpec as P

TERMS = 8
LATTICE = 0.25
CORES = 2


def exchange(pieces, axes):
    return lax.all_to_all(pieces, axes, split_axis=0, concat_axis=0, tiled=True)


def from_everyone(shard, axes):
    count = math.prod(lax.axis_size(axis) for axis in axes)
    return exchange(jnp.broadcast_to(shard, (count, *shard.shape)), axes)


def term_kernel(order, parts_ref, weight_ref, accum_ref, term_ref, total_ref, product):
    step = pl.program_id(0)
    span = parts_ref.shape[0]
    layers, lines = weight_ref.shape[1:3]
    rows = lines // span

    @pl.when(step == 0)
    def _():
        product[...] = jnp.zeros_like(product)

    for first in range(0, layers, 2):
        total = None
        for pair in range(0, span, 2):
            left = jnp.concatenate([parts_ref[x] for x in (pair, pair + 1)], axis=1)
            right = jnp.concatenate(
                [
                    jnp.concatenate(
                        [
                            weight_ref[side, layer, x * rows : (x + 1) * rows, :]
                            for x in (pair, pair + 1)
                            for side in range(CORES)
                        ],
                        axis=0,
                    )
                    for layer in (first, first + 1)
                ],
                axis=1,
            )
            part = jnp.dot(left, right, preferred_element_type=jnp.float32)
            total = part if total is None else total + part
        width = total.shape[1]
        at = first // 2 * width
        product[:, at : at + width] += total

    @pl.when(step == pl.num_programs(0) - 1)
    def _():
        term = (product[...] / order).astype(jnp.bfloat16)
        term_ref[...] = term
        total_ref[...] = accum_ref[...] + term.astype(jnp.float32)


def next_term(order, parts, weight, accum):
    groups, cores, layers, lines, twice = weight.shape
    span, count, width = parts.shape
    whole = pl.BlockSpec((count, width), lambda step: (0, 0))
    return pl.pallas_call(
        functools.partial(term_kernel, order),
        grid=(groups,),
        in_specs=[
            pl.BlockSpec((span, count, twice), lambda step: (0, 0, step)),
            pl.BlockSpec((None, cores, layers, lines, twice), lambda step: (step, 0, 0, 0, 0)),
            whole,
        ],
        out_specs=[whole, whole],
        out_shape=[
            jax.ShapeDtypeStruct((count, width), jnp.bfloat16),
            jax.ShapeDtypeStruct((count, width), jnp.float32),
        ],
        scratch_shapes=[pltpu.VMEM((count, width), jnp.float32)],
        compiler_params=pltpu.CompilerParams(dimension_semantics=("arbitrary",)),
        name="series_term",
    )(parts, weight, accum)


def per_device(intersection_re, intersection_im, weights, shells, rotation):
    groups = lax.axis_size("z")
    span = lax.axis_size("col")
    layers = lax.axis_size("depth")
    core = lax.axis_index("core")
    layer = lax.axis_index("depth")
    rows, width = intersection_re.shape[1:]
    block = width // groups
    position = lax.axis_index(("z", "core", "col"))

    eye = jnp.eye(rows, dtype=bool)

    def diagonal_of(values):
        square = lax.dynamic_slice_in_dim(values[0], position * rows, rows, 1)
        return jnp.sum(jnp.where(eye, square.astype(jnp.float32), 0.0), axis=0)

    piece = jnp.stack([diagonal_of(intersection_re), diagonal_of(intersection_im)]).astype(jnp.bfloat16)
    raw = jnp.stack([intersection_re[0], intersection_im[0]]).reshape(2, rows, groups, block)
    raw = jnp.moveaxis(raw, 2, 0)
    own_columns = from_everyone(piece, ("depth",))
    raw, own_columns = lax.optimization_barrier((raw, own_columns))
    raw = exchange(raw, "depth")
    diagonals = from_everyone(own_columns, ("z", "core", "col"))
    diagonals = diagonals.reshape(groups, -1, layers, 2, rows)
    diagonals = lax.dynamic_index_in_dim(diagonals, layer, 0, keepdims=False)
    diagonals = jnp.moveaxis(diagonals, 0, 2).reshape(layers, 2, block).astype(jnp.float32)
    diag_re = diagonals[:, 0]
    diag_im = diagonals[:, 1]
    vectors = shells.astype(jnp.float32) * LATTICE
    phase = jnp.arctan2(diag_im, diag_re)
    centre = -jnp.sum((weights[:, None] * vectors)[:, :, None] * phase[:, None, :], axis=0)
    spread = phase + jnp.sum(vectors[:, :, None] * centre[None], axis=1)
    ratio = spread / (diag_re * diag_re + diag_im * diag_im)
    scale_re = weights[:, None] * (diag_re + ratio * diag_im)
    scale_im = weights[:, None] * (diag_im - ratio * diag_re)

    raw = raw.astype(jnp.float32)
    grad = jnp.sum(raw[:, 0] * scale_re[:, None, :] + raw[:, 1] * scale_im[:, None, :], axis=0)

    direct = jnp.moveaxis(grad.reshape(rows, CORES, span, rows), 2, 0).reshape(span, rows, CORES * rows)
    direct = exchange(direct, "col").reshape(span * rows, CORES * rows)
    sides = grad.reshape(rows, CORES, span * rows)
    mirror = []
    for crossed in range(CORES):
        pairs = [
            ((z * CORES + c) * layers + y, (y * CORES + (c ^ crossed)) * layers + z)
            for z in range(groups)
            for c in range(CORES)
            for y in range(layers)
        ]
        half = lax.dynamic_index_in_dim(sides, core ^ crossed, 1, keepdims=False)
        mirror.append(lax.ppermute(half, ("z", "core", "depth"), pairs))
    lower = jnp.where(core == 0, mirror[0], mirror[1])
    upper = jnp.where(core == 0, mirror[1], mirror[0])
    mirrored = jnp.concatenate([lower, upper], axis=0).T
    factor = 1.25 / math.sqrt(weights.shape[0])
    operator = ((direct - mirrored) * factor).astype(jnp.bfloat16)
    operator = from_everyone(operator, ("depth",))
    operator = lax.all_gather(operator, ("z", "core"), axis=0, tiled=False)
    operator = operator.reshape(groups, CORES, layers, span * rows, CORES * rows)

    share = rows // layers
    own_rows = lax.dynamic_slice_in_dim(rotation, layer * share, share, 0)
    term = from_everyone(own_rows, ("col",)).reshape(span * share, groups * CORES, span, rows)
    parts = jnp.moveaxis(term, 2, 0).reshape(span, span * share, -1)
    accum = lax.dynamic_index_in_dim(parts, lax.axis_index("col"), 0, keepdims=False).astype(jnp.float32)
    for order in range(1, TERMS):
        term, accum = next_term(order, parts, operator, accum)
        if order + 1 < TERMS:
            parts = from_everyone(term, ("col",))

    out = jnp.moveaxis(accum.reshape(span, share, layers, CORES * rows), 2, 1)
    out = exchange(out.reshape(span * layers, share, CORES * rows), ("col", "depth"))
    out = out.reshape(span, layers, share, CORES, rows)
    return jnp.transpose(out, (1, 2, 3, 0, 4)).reshape(rows, block)


def solution(mesh):
    row, col, depth = mesh.devices.shape
    finer = Mesh(mesh.devices.reshape(row // CORES, CORES, col, depth), ("z", "core", "col", "depth"))
    lines = ("z", "core", "col")
    return jax.shard_map(
        per_device,
        mesh=finer,
        in_specs=(P("depth", lines, None), P("depth", lines, None), P(), P(), P(lines, None)),
        out_specs=P(lines, "depth"),
        check_vma=False,
    )
```
